32 devices in a mesh: cls: 32 (over z, y, x, core).
Axes of the slice: x: 2, y: 2, z: 4, core: 2. Of those that a mesh axis runs over, the one named last changes fastest.
Arguments:
- features: bfloat16 [512, 12544], P('cls'), may hold values from -6 to 6
- fc_weight: bfloat16 [12544, 512], replicated, may hold values from -0.0546875 to 0.0546875
- centers: bfloat16 [131072, 512], P('cls'), may hold values from -6 to 6
- labels: int32 [512], replicated, may hold values from 0 to 131071
Outputs:
- loss: float32 [512], P('cls')
- grad_centers: bfloat16 [131072, 512], P('cls')
- grad_fc: float32 [12544, 512], P('cls')
The draws below stay inside these ranges and needn't reach their ends.
All inputs are finite; a program needn't handle non-finite values.
Results may differ from the reference program's by a relative error of at most 0.0078.
Values may be sent and summed in bfloat16 or wider, within the bound.
A program may use at most 128 MiB of HBM per device.

```python
import math
import jax
import jax.numpy as jnp
from jax import lax

D = 512
F = 12544
C_DEV = 4096
B = 512
C = 131072
N_CLS = 32


def place_ends(entries, own_key, least, top_value):
    longest = entries.shape.index(max(entries.shape))
    spots = []
    for shift in (0, 1):
        where = [jax.random.randint(jax.random.fold_in(own_key, axis), (), 0, length) for axis, length in enumerate(entries.shape)]
        where[longest] = (where[longest] + shift) % entries.shape[longest]
        spots.append(tuple(where))
    return entries.at[spots[0]].set(least).at[spots[1]].set(top_value)


def levels(key, shape, cuts, smallest, largest):
    level, own = 1.0, jax.random.fold_in(key, 6)
    for position, blocks in cuts:
        steps = jnp.exp(jax.random.uniform(jax.random.fold_in(own, position), (blocks,), jnp.float32, smallest / len(cuts), largest / len(cuts)))
        level = level * jnp.repeat(steps, shape[position] // blocks).reshape([-1 if axis == position else 1 for axis in range(len(shape))])
    return level


def gaussian(key, shape, deviation, reach, split=(), held_as=jnp.bfloat16):
    result = deviation * jax.random.normal(key, shape, jnp.float32)
    if split:
        result = result * levels(key, shape, split, -0.22, 0.18)
    return jnp.clip(result, -reach, reach).astype(held_as)


def setup_inputs(seed: int = 0) -> dict:
    key_list = jax.random.split(jax.random.key(seed), 5)
    return {
        "features": gaussian(key_list[0], (B, F), 1.0, 6.0, ((0, 32),)),
        "fc_weight": gaussian(key_list[1], (F, D), F ** -0.5, 0.0546875),
        "centers": gaussian(key_list[2], (C, D), 1.0, 6.0, ((0, 32),)),
        "labels": place_ends(jax.random.randint(key_list[3], (B,), 0, C), jax.random.fold_in(key_list[3], 1), 0, C - 1).astype(jnp.int32),
    }


logit_scale = 64.0
cos_margin = math.cos(0.5)
sin_margin = math.sin(0.5)
epsilon = 1e-06

def inverse_norm(values):
    return lax.rsqrt(lax.optimization_barrier(jnp.sum(values * values, axis=1, keepdims=True)) + epsilon)

def margin_logits(emb_low, center_low, labels, offset):
    cosines = jnp.dot(emb_low, center_low.T, preferred_element_type=jnp.float32)
    local_ids = labels - offset
    is_target = local_ids[:, None] == lax.broadcasted_iota(jnp.int32, (1, center_low.shape[0]), 1)
    target_cos = lax.optimization_barrier(jnp.sum(jnp.where(is_target, cosines, 0.0), axis=1))
    target_sine = jnp.sqrt(1.0 - target_cos * target_cos)
    margined = target_cos * cos_margin - target_sine * sin_margin
    logits = logit_scale * jnp.where(is_target, margined[:, None], cosines)
    slope = cos_margin + sin_margin * target_cos / target_sine
    return (logits, is_target, slope)

def center_parts(block):
    center_float = block.astype(jnp.float32)
    inv_center = inverse_norm(center_float)
    center_dir = center_float * inv_center
    return (inv_center, center_dir, center_dir.astype(jnp.bfloat16))

def reference(features, fc_weight, centers, labels):
    batch = labels.shape[0]
    embedded = jnp.dot(features, fc_weight, preferred_element_type=jnp.float32).astype(jnp.bfloat16)
    emb_float = embedded.astype(jnp.float32)
    inv_emb = inverse_norm(emb_float)
    emb_dir = emb_float * inv_emb
    emb_low = emb_dir.astype(jnp.bfloat16)
    blocks = centers.reshape(N_CLS, C_DEV, D)
    shard_ids = jnp.arange(N_CLS, dtype=jnp.int32)

    def stats_step(carry, item):
        shard, block = item
        unused_inv, unused_dir, center_low = center_parts(block)
        logits, is_target, unused_slope = margin_logits(emb_low, center_low, labels, shard * C_DEV)
        running_sum, target_sum = carry
        running_sum = running_sum + lax.optimization_barrier(jnp.sum(jnp.exp(logits - logit_scale), axis=1))
        target_sum = target_sum + lax.optimization_barrier(jnp.sum(jnp.where(is_target, logits, 0.0), axis=1))
        return ((running_sum, target_sum), None)
    start_stats = (jnp.zeros((batch,), jnp.float32), jnp.zeros((batch,), jnp.float32))
    (row_sum, target_sum), unused_out = lax.scan(stats_step, start_stats, (shard_ids, blocks))
    log_total = logit_scale + jnp.log(row_sum)
    loss = log_total - target_sum

    def grad_step(grad_dir, item):
        shard, block = item
        inv_center, center_dir, center_low = center_parts(block)
        logits, is_target, slope = margin_logits(emb_low, center_low, labels, shard * C_DEV)
        probs = jnp.exp(logits - log_total[:, None])
        grad_cos = (logit_scale * (probs - is_target.astype(jnp.float32)) * jnp.where(is_target, slope[:, None], 1.0)).astype(jnp.bfloat16)
        grad_unit = jnp.dot(grad_cos.T, emb_low, preferred_element_type=jnp.float32)
        grad_center = ((grad_unit - center_dir * lax.optimization_barrier(jnp.sum(grad_unit * center_dir, axis=1, keepdims=True))) * inv_center).astype(jnp.bfloat16)
        grad_dir = grad_dir + jnp.dot(grad_cos, center_low, preferred_element_type=jnp.float32)
        return (grad_dir, grad_center)
    grad_dir, grad_blocks = lax.scan(grad_step, jnp.zeros((batch, D), jnp.float32), (shard_ids, blocks))
    grad_centers = grad_blocks.reshape(N_CLS * C_DEV, D)
    grad_emb = ((grad_dir - emb_dir * lax.optimization_barrier(jnp.sum(grad_dir * emb_dir, axis=1, keepdims=True))) * inv_emb).astype(jnp.bfloat16)
    grad_fc = jnp.dot(features.T, grad_emb, preferred_element_type=jnp.float32)
    return (loss, grad_centers, grad_fc)
```

```python
import functools
import math

import jax
import jax.numpy as jnp
from jax import lax
from jax.experimental import pallas as pl
from jax.experimental.pallas import tpu as pltpu
from jax.sharding import PartitionSpec as P

logit_scale = 64.0
cos_margin = math.cos(0.5)
sin_margin = math.sin(0.5)
epsilon = 1e-06
exp2_scale = logit_scale * math.log2(math.e)
lanes = 128
MESH = pl.DeviceIdType.MESH
f32, bf16 = jnp.float32, jnp.bfloat16


def inverse_norm(values):
    return lax.rsqrt(jnp.sum(values * values, axis=1, keepdims=True) + epsilon)


def largest_divisor(number, most):
    return next(d for d in range(most, 0, -1) if number % d == 0)


def repeat(count, body, unroll):
    if unroll:
        for k in range(count):
            body(k)
    else:
        lax.fori_loop(0, count, lambda k, carry: (body(k), carry)[1], 0)


def ds(k, size):
    return pl.ds(k * size if isinstance(k, int) else pl.multiple_of(k * size, size), size)


def row_sums(values):
    part = values[:, :lanes]
    for j in range(1, values.shape[1] // lanes):
        part = part + values[:, j * lanes : (j + 1) * lanes]
    return jnp.sum(part.T, axis=0, keepdims=True)


def column(row):
    return jnp.broadcast_to(row, (lanes, row.shape[1])).T


def main_kernel(
    n, rows, slots, feat_hbm, weight, centers_hbm, labels,
    loss_out, gc_out, features_out, grads_out,
    feat, wbuf, cbuf, clow, inv_c, expo, sums, acc, target, esend, emb, scaled,
    lab, tfix, fsend, ssend, srecv, psend, pair, precv, gsend,
    fsem, wsem, csem, ssems, rsems,
):
    me = lax.axis_index("cls")
    tok, feats = feat.shape
    classes, width = cbuf.shape
    batch = n * tok
    chunk = wbuf.shape[1]
    chunks = feats // chunk
    blocks = classes // rows
    part = feats // n
    half = n // 2
    core = lax.rem(me, 2)
    chip = me // 2
    partner = me + 1 - 2 * core
    side = me // half
    near, far = side * half, (1 - side) * half
    unroll = batch <= 512
    group = min(batch, 512)
    frecv, grecv = features_out, grads_out

    pieces = largest_divisor(chunks, 14)
    piece = feats // pieces

    def feat_copy(c):
        at = pl.ds(c * piece, piece)
        return pltpu.make_async_copy(feat_hbm.at[:, at], feat.at[:, at], fsem)

    def weight_copy(c):
        return pltpu.make_async_copy(
            weight.at[pl.ds(c * chunk, chunk)], wbuf.at[c % slots], wsem.at[c % slots]
        )

    ahead = min(slots, 6)
    for c in range(pieces):
        feat_copy(c).start()
    for c in range(min(ahead, chunks)):
        weight_copy(c).start()
    centers_copy = pltpu.make_async_copy(centers_hbm, cbuf, csem)

    barrier = pltpu.get_barrier_semaphore()

    def greet(i, carry):
        pl.semaphore_signal(barrier, inc=1, device_id=(lax.rem(me + i, n),), device_id_type=MESH)
        return carry

    lax.fori_loop(1, n, greet, 0)

    def send_features(base, first, last):
        def step(i, carry):
            dst = base + lax.rem(me + i, half)
            pltpu.make_async_remote_copy(
                src_ref=fsend.at[dst], dst_ref=frecv.at[me],
                send_sem=ssems.at[1], recv_sem=rsems.at[1],
                device_id=(dst,), device_id_type=MESH,
            ).start()
            return carry

        lax.fori_loop(first, last, step, 0)

    def send_all(phase, source, target):
        def step(i, carry):
            dst = lax.rem(me + i, n)
            pltpu.make_async_remote_copy(
                src_ref=source, dst_ref=target.at[me],
                send_sem=ssems.at[phase], recv_sem=rsems.at[phase],
                device_id=(dst,), device_id_type=MESH,
            ).start()
            return carry

        lax.fori_loop(1, n, step, 0)

    def wait_all(sems, phase, target, count):
        whole = target.at[pl.ds(0, count)]
        pltpu.make_async_copy(whole, whole, sems.at[phase]).wait()

    def send_chips(phase, source, target, slot):
        def step(i, carry):
            to = lax.rem(chip + i, half)
            pltpu.make_async_remote_copy(
                src_ref=source(to), dst_ref=target.at[slot],
                send_sem=ssems.at[phase], recv_sem=rsems.at[phase],
                device_id=(2 * to + core,), device_id_type=MESH,
            ).start()
            return carry

        lax.fori_loop(1, half, step, 0)

    def send_partner(phase, source, target):
        def step(j, carry):
            pltpu.make_async_remote_copy(
                src_ref=source(j), dst_ref=target(j),
                send_sem=ssems.at[phase], recv_sem=rsems.at[phase],
                device_id=(partner,), device_id_type=MESH,
            ).start()
            return carry

        lax.fori_loop(0, half, step, 0)

    pltpu.make_async_copy(feat_hbm, feat, fsem).wait()
    for j in range(n):
        fsend[j] = feat[:, j * part : (j + 1) * part]
    frecv[me] = fsend[me]
    local = labels[...] - me * classes
    lab[...] = column(local.astype(f32)).astype(jnp.int32)
    total = jnp.zeros((tok, width), f32)
    for c in range(chunks):
        if c == min(3, chunks - 1):
            pl.semaphore_wait(barrier, n - 1)
            send_features(far, 0, half // 2)
        weight_copy(c).wait()
        total = total + jnp.dot(
            feat[:, c * chunk : (c + 1) * chunk], wbuf[c % slots], preferred_element_type=f32
        )
        if c + ahead < chunks:
            weight_copy(c + ahead).start()
        if c == max(chunks - ahead, 0):
            centers_copy.start()
    esend[...] = total.astype(bf16)
    emb[me] = total.astype(bf16)
    send_chips(0, lambda to: esend, emb, me)

    centers_copy.wait()

    def normalise(k):
        at = ds(k, rows)
        block = cbuf[at].astype(f32)
        inv = inverse_norm(block)
        inv_c[at] = jnp.broadcast_to(inv, (rows, lanes))
        clow[at] = (block * inv).astype(bf16)

    repeat(blocks, normalise, unroll)

    def hits(g, first):
        ids = lax.broadcasted_iota(jnp.int32, (group, lanes), 1) + first
        return ids == lab[ds(g, group)]

    def find_targets(g):
        def block(k):
            chosen = jnp.concatenate(
                [
                    jnp.where(hits(g, k * rows + j * lanes), 1.0, 0.0).astype(bf16)
                    for j in range(rows // lanes)
                ],
                axis=1,
            )
            acc[ds(g, group)] += jnp.dot(chosen, clow[ds(k, rows)], preferred_element_type=f32)

        acc[ds(g, group)] = jnp.zeros((group, width), f32)
        repeat(blocks, block, unroll)
        target[ds(g, group)] = acc[ds(g, group)].astype(bf16)

    repeat(batch // group, find_targets, unroll)

    wait_all(rsems, 0, emb, half - 1)
    send_partner(5, lambda j: emb.at[2 * j + core], lambda j: emb.at[2 * j + core])
    send_features(far, half // 2, half)
    wait_all(rsems, 5, emb, half)
    wait_all(ssems, 5, emb, half)

    all_emb = emb[...].reshape(batch, width).astype(f32)
    emb_low = (all_emb * inverse_norm(all_emb)).astype(bf16)
    emb[...] = emb_low.reshape(n, tok, width)
    tcos = row_sums(emb_low.astype(f32) * target[...].astype(f32))
    mine = (local >= 0) & (local < classes)
    tsin = jnp.sqrt(1.0 - tcos * tcos)
    tlogit = logit_scale * (tcos * cos_margin - tsin * sin_margin)
    slope = cos_margin + sin_margin * tcos / tsin
    texp = jnp.exp(tlogit)

    def forward(g):
        picked = emb[ds(g, group // tok)].reshape(group, width)
        sums[ds(g, group)] = jnp.zeros((group, lanes), f32)

        def block(k):
            cos = lax.dot_general(
                picked, clow[ds(k, rows)], (((1,), (1,)), ((), ())), preferred_element_type=f32
            )
            row = jnp.zeros((group, lanes), f32)
            for j in range(rows // lanes):
                power = jnp.exp2(exp2_scale * cos[:, j * lanes : (j + 1) * lanes])
                power = jnp.where(hits(g, k * rows + j * lanes), 0.0, power)
                row = row + power
                expo[ds(g, group), ds(k * (rows // lanes) + j, lanes)] = power.astype(bf16)
            sums[ds(g, group)] += row

        repeat(blocks, block, unroll)

    repeat(batch // group, forward, unroll)
    ssend[0:1] = row_sums(sums[...]) + jnp.where(mine, texp, 0.0)
    ssend[1:2] = jnp.where(mine, tlogit, 0.0)
    srecv[me] = ssend[...]
    send_all(2, ssend, srecv)

    def weigh(g):
        acc[ds(g, 256)] = jnp.dot(expo[ds(g, 256)], clow[...], preferred_element_type=f32)

    repeat(batch // 256, weigh, unroll)
    wait_all(rsems, 2, srecv, n - 1)
    stats = jnp.sum(srecv[...], axis=0)
    norm = stats[0:1]
    loss_row = jnp.log(norm) - stats[1:2]
    tgrad = jnp.where(mine, logit_scale * (texp / norm - 1.0) * slope, 0.0)
    scale = column(logit_scale / norm)
    tscale = column(tgrad)
    tfix[...] = column((texp - norm) * slope)

    for j in range(width // lanes):
        at = slice(j * lanes, (j + 1) * lanes)
        total = scale * acc[:, at] + tscale * target[:, at].astype(f32)
        acc[:, at] = total
        psend[:, :, at] = total.astype(bf16).reshape(n, tok, lanes)
    send_partner(6, lambda j: psend.at[2 * j + 1 - core], lambda j: pair.at[j])
    own_row = lax.broadcasted_iota(jnp.int32, (tok, batch), 0) + me * tok
    own_lane = lax.broadcasted_iota(jnp.int32, (tok, batch), 1)
    picked_loss = jnp.where(own_row == own_lane, loss_row, 0.0)
    loss_out[...] = row_sums(picked_loss)
    for j in range(width // lanes):
        at = slice(j * lanes, (j + 1) * lanes)
        low = emb[:, :, at].reshape(batch, lanes).astype(f32)
        scaled[:, at] = (low * scale).astype(bf16)
    wait_all(rsems, 6, pair, half)

    def add_pair(j, carry):
        at = pl.ds(pl.multiple_of((2 * j + core) * tok, tok), tok)
        psend[2 * j + core] = (acc[at] + pair[j].astype(f32)).astype(bf16)
        return carry

    lax.fori_loop(0, half, add_pair, 0)
    precv[chip] = psend[me]
    send_chips(3, lambda to: psend.at[2 * to + core], precv, chip)
    send_features(near, 1, half)

    ones = jnp.ones((width, lanes), bf16)

    def center_grads(k, carry):
        at = ds(k, rows)
        weights = []
        for j in range(rows // lanes):
            block = expo[:, ds(k * (rows // lanes) + j, lanes)].astype(f32)
            ids = lax.broadcasted_iota(jnp.int32, (batch, lanes), 1) + (k * rows + j * lanes)
            weights.append(jnp.where(ids == lab[...], tfix[...], block).astype(bf16))
        unit = lax.dot_general(
            jnp.concatenate(weights, axis=1), scaled[...], (((0,), (0,)), ((), ())),
            preferred_element_type=f32,
        )
        center = cbuf[at].astype(f32)
        along = jnp.dot((unit * center).astype(bf16), ones, preferred_element_type=f32)
        inv = inv_c[at]
        along = along * (inv * inv * inv)
        for j in range(width // lanes):
            cols = slice(j * lanes, (j + 1) * lanes)
            gc_out[at, cols] = (unit[:, cols] * inv - center[:, cols] * along).astype(bf16)
        return carry

    early = 5 * blocks // 8
    lax.fori_loop(0, early, center_grads, 0)

    wait_all(rsems, 3, precv, half - 1)
    grad_dir = jnp.sum(precv[...].astype(f32), axis=0)
    own = esend[...].astype(f32)
    inv_emb = inverse_norm(own)
    emb_dir = own * inv_emb
    along = jnp.sum(grad_dir * emb_dir, axis=1, keepdims=True)
    grad_emb = ((grad_dir - emb_dir * along) * inv_emb).astype(bf16)
    gsend[...] = grad_emb
    grecv[me] = grad_emb
    send_chips(4, lambda to: gsend, grecv, me)
    lax.fori_loop(early, blocks, center_grads, 0)

    wait_all(rsems, 1, frecv, n - 1)
    wait_all(rsems, 4, grecv, half - 1)
    send_partner(7, lambda j: grecv.at[2 * j + core], lambda j: grecv.at[2 * j + core])
    wait_all(ssems, 0, emb, half - 1)
    wait_all(ssems, 1, frecv, n - 1)
    wait_all(ssems, 2, srecv, n - 1)
    wait_all(ssems, 3, precv, half - 1)
    wait_all(ssems, 4, grecv, half - 1)
    wait_all(ssems, 6, pair, half)
    wait_all(rsems, 7, grecv, half)
    wait_all(ssems, 7, grecv, half)


def last_kernel(gc, features, grads, loss, loss_out, gc_out, fc_out, stage, sems):
    gc_copy = pltpu.make_async_copy(gc, gc_out, sems.at[0])
    gc_copy.start()
    n, tok, part = features.shape
    stage[...] = lax.dot_general(
        features[...].reshape(n * tok, part), grads[...].reshape(n * tok, grads.shape[2]),
        (((0,), (0,)), ((), ())), preferred_element_type=f32,
    )
    fc_copy = pltpu.make_async_copy(stage, fc_out, sems.at[1])
    fc_copy.start()
    loss_out[...] = loss[0]
    gc_copy.wait()
    fc_copy.wait()


def on_device(features, fc_weight, centers, labels):
    n = lax.axis_size("cls")
    tok, feats = features.shape
    classes, width = centers.shape
    batch = labels.shape[0]
    rows = 256
    chunk = lanes * largest_divisor(feats // lanes, 7)
    slots = feats // chunk if batch <= 1024 else 2
    part = feats // n
    vmem = pl.BlockSpec(memory_space=pltpu.VMEM)
    hbm = pl.BlockSpec(memory_space=pl.ANY)
    loss, gc, spread, grads = pl.pallas_call(
        functools.partial(main_kernel, n, rows, slots),
        out_shape=(
            pltpu.VMEM((1, tok), f32),
            pltpu.VMEM((classes, width), bf16),
            pltpu.VMEM((n, tok, part), bf16),
            pltpu.VMEM((n, tok, width), bf16),
        ),
        in_specs=[hbm, hbm, hbm, vmem],
        out_specs=(vmem, vmem, vmem, vmem),
        scratch_shapes=[
            pltpu.VMEM((tok, feats), bf16),
            pltpu.VMEM((slots, chunk, width), bf16),
            pltpu.VMEM((classes, width), bf16),
            pltpu.VMEM((classes, width), bf16),
            pltpu.VMEM((classes, lanes), f32),
            pltpu.VMEM((batch, classes), bf16),
            pltpu.VMEM((batch, lanes), f32),
            pltpu.VMEM((batch, width), f32),
            pltpu.VMEM((batch, width), bf16),
            pltpu.VMEM((tok, width), bf16),
            pltpu.VMEM((n, tok, width), bf16),
            pltpu.VMEM((batch, width), bf16),
            pltpu.VMEM((batch, lanes), jnp.int32),
            pltpu.VMEM((batch, lanes), f32),
            pltpu.VMEM((n, tok, part), bf16),
            pltpu.VMEM((2, batch), f32),
            pltpu.VMEM((n, 2, batch), f32),
            pltpu.VMEM((n, tok, width), bf16),
            pltpu.VMEM((n // 2, tok, width), bf16),
            pltpu.VMEM((n // 2, tok, width), bf16),
            pltpu.VMEM((tok, width), bf16),
            pltpu.SemaphoreType.DMA,
            pltpu.SemaphoreType.DMA((slots,)),
            pltpu.SemaphoreType.DMA,
            pltpu.SemaphoreType.DMA((8,)),
            pltpu.SemaphoreType.DMA((8,)),
        ],
        compiler_params=pltpu.CompilerParams(
            collective_id=0, has_side_effects=True, vmem_limit_bytes=54 * 2**20
        ),
    )(features, fc_weight, centers, labels[None])
    return pl.pallas_call(
        last_kernel,
        out_shape=(
            jax.ShapeDtypeStruct((tok,), f32),
            jax.ShapeDtypeStruct((classes, width), bf16),
            jax.ShapeDtypeStruct((part, width), f32),
        ),
        in_specs=[vmem, vmem, vmem, vmem],
        out_specs=(vmem, hbm, hbm),
        scratch_shapes=[pltpu.VMEM((part, width), f32), pltpu.SemaphoreType.DMA((2,))],
        compiler_params=pltpu.CompilerParams(vmem_limit_bytes=8 * 2**20),
    )(gc, spread, grads, loss)


def solution(mesh):
    placed = (P("cls", None), P(), P("cls", None), P())
    return jax.shard_map(
        on_device,
        mesh=mesh,
        in_specs=placed,
        out_specs=(P("cls"), P("cls", None), P("cls", None)),
        check_vma=False,
    )
```

```python
import functools
import math

import jax
import jax.numpy as jnp
from jax import lax
from jax.experimental import pallas as pl
from jax.experimental.pallas import tpu as pltpu
from jax.sharding import PartitionSpec as P

logit_scale = 64.0
cos_margin = math.cos(0.5)
sin_margin = math.sin(0.5)
epsilon = 1e-06
exp2_scale = logit_scale * math.log2(math.e)
lanes = 128
MESH = pl.DeviceIdType.MESH
f32, bf16 = jnp.float32, jnp.bfloat16


def inverse_norm(values):
    return lax.rsqrt(jnp.sum(values * values, axis=1, keepdims=True) + epsilon)


def largest_divisor(number, most):
    return next(d for d in range(most, 0, -1) if number % d == 0)


def repeat(count, body, unroll):
    if unroll:
        for k in range(count):
            body(k)
    else:
        lax.fori_loop(0, count, lambda k, carry: (body(k), carry)[1], 0)


def ds(k, size):
    return pl.ds(k * size if isinstance(k, int) else pl.multiple_of(k * size, size), size)


def row_sums(values):
    part = values[:, :lanes]
    for j in range(1, values.shape[1] // lanes):
        part = part + values[:, j * lanes : (j + 1) * lanes]
    return jnp.sum(part.T, axis=0, keepdims=True)


def column(row):
    return jnp.broadcast_to(row, (lanes, row.shape[1])).T


def main_kernel(
    n, rows, slots, split, feat_hbm, weight, centers_hbm, labels,
    loss_out, gc_out, features_out, grads_out,
    feat, wbuf, cbuf, clow, inv_c, expo, sums, acc, target, esend, emb, low,
    lab, tfix, fsend, ssend, srecv, psend, pair, tpair, blocks_u, blocks_t,
    far_u, near_u, far_t, near_t, fold_send, fold_recv, gsend,
    fsem, wsem, csem, ssems, rsems,
):
    me = lax.axis_index("cls")
    tok, feats = feat.shape
    classes, width = cbuf.shape
    batch = n * tok
    chunk = wbuf.shape[1]
    chunks = feats // chunk
    blocks = classes // rows
    part = feats // n
    half = n // 2
    quarter = n // 4
    core = lax.rem(me, 2)
    chip = me // 2
    partner = me + 1 - 2 * core
    mirror = lax.rem(me + half, n)
    side = me // half
    near, far = side * half, (1 - side) * half
    place = chip - side * quarter
    unroll = batch <= 512
    group = min(batch // 2, 512)
    groups = batch // 2 // group
    frecv, grecv = features_out, grads_out

    def feat_copy(c):
        at = pl.ds(c * chunk, chunk)
        return pltpu.make_async_copy(feat_hbm.at[:, at], feat.at[:, at], fsem.at[c])

    def weight_start(c):
        size = chunk // split
        for i in range(split):
            pltpu.make_async_copy(
                weight.at[pl.ds(c * chunk + i * size, size)],
                wbuf.at[c % slots, pl.ds(i * size, size)],
                wsem.at[c % slots],
            ).start()

    def weight_wait(c):
        pltpu.make_async_copy(
            weight.at[pl.ds(c * chunk, chunk)], wbuf.at[c % slots], wsem.at[c % slots]
        ).wait()

    barrier = pltpu.get_barrier_semaphore()

    def greet(i, carry):
        pl.semaphore_signal(barrier, inc=1, device_id=(lax.rem(me + i, n),), device_id_type=MESH)
        return carry

    ahead = 4 if slots == chunks else slots
    feat_copy(0).start()
    weight_start(0)
    lax.fori_loop(1, n, greet, 0)
    for c in range(1, chunks):
        feat_copy(c).start()
        if c < ahead:
            weight_start(c)

    def send(phase, source, target_ref, to):
        pltpu.make_async_remote_copy(
            src_ref=source, dst_ref=target_ref,
            send_sem=ssems.at[phase], recv_sem=rsems.at[phase],
            device_id=(to,), device_id_type=MESH,
        ).start()

    def loop(first, last, body):
        lax.fori_loop(first, last, lambda i, carry: (body(i), carry)[1], 0)

    def wait_all(sems, phase, target_ref, count):
        whole = target_ref.at[pl.ds(0, count)]
        pltpu.make_async_copy(whole, whole, sems.at[phase]).wait()

    def mate(i):
        to = lax.rem(place + i, quarter)
        return to, near + 2 * to + core

    def spread_start(phase, own, whole):
        send(phase, own, whole.at[me], mirror)
        loop(1, quarter, lambda i: send(phase + 1, own, whole.at[me], mate(i)[1]))

    def spread_relay(phase, whole):
        wait_all(rsems, phase, whole, 1)
        block = whole.at[mirror]
        loop(1, quarter, lambda i: send(phase + 2, block, block, mate(i)[1]))

    def spread_near(phase, whole):
        wait_all(rsems, phase + 1, whole, quarter - 1)

        def one(j):
            block = whole.at[near + 2 * j + core]
            send(phase + 3, block, block, partner)

        loop(0, quarter, one)

    def spread_far(phase, whole):
        wait_all(rsems, phase + 2, whole, quarter - 1)

        def one(j):
            block = whole.at[far + 2 * j + core]
            send(phase + 4, block, block, partner)

        loop(0, quarter, one)

    def spread_end(phase, whole):
        for i, count in enumerate((1, quarter - 1, quarter - 1, quarter, quarter)):
            wait_all(ssems, phase + i, whole, count)

    def fold_far(phase, parts, buf):
        def one(i):
            to, device = mate(i)
            send(phase, parts.at[(1 - side) * quarter + to], buf.at[place], device)

        loop(1, quarter, one)
        buf[place] = parts[(1 - side) * quarter + place]

    def fold_near(phase, parts, buf):
        def one(i):
            to, device = mate(i)
            send(phase, parts.at[side * quarter + to], buf.at[place], device)

        loop(1, quarter, one)
        buf[place] = parts[chip]

    def fold_cross(phase, far_buf, which):
        wait_all(rsems, phase, far_buf, quarter - 1)
        fold_send[which] = jnp.sum(far_buf[...].astype(f32), axis=0).astype(bf16)
        send(phase + 2, fold_send.at[which], fold_recv.at[which], mirror)

    def fold_end(phase, near_buf, which):
        wait_all(rsems, phase + 1, near_buf, quarter - 1)
        wait_all(rsems, phase + 2, near_buf, 1)
        for i, count in enumerate((quarter - 1, quarter - 1, 1)):
            wait_all(ssems, phase + i, near_buf, count)
        return jnp.sum(near_buf[...].astype(f32), axis=0) + fold_recv[which].astype(f32)

    total = jnp.zeros((tok, width), f32)
    for c in range(chunks):
        feat_copy(c).wait()
        weight_wait(c)
        if slots == chunks and c + ahead < chunks:
            weight_start(c + ahead)
        total = total + jnp.dot(
            feat[:, c * chunk : (c + 1) * chunk], wbuf[c % slots], preferred_element_type=f32
        )
        if slots < chunks and c + ahead < chunks:
            weight_start(c + ahead)
        if c == max(chunks - ahead, 0):
            for i in range(4):
                at = pl.ds(i * (classes // 4), classes // 4)
                pltpu.make_async_copy(centers_hbm.at[at], cbuf.at[at], csem).start()
    esend[...] = total.astype(bf16)
    emb[me] = total.astype(bf16)
    pl.semaphore_wait(barrier, n - 1)
    spread_start(0, esend, emb)
    for j in range(n):
        fsend[j] = feat[:, j * part : (j + 1) * part]
    frecv[me] = fsend[me]
    local = labels[...] - me * classes
    lab[...] = column(local.astype(f32)).astype(jnp.int32)

    pltpu.make_async_copy(centers_hbm, cbuf, csem).wait()

    def normalise(k):
        at = ds(k, rows)
        block = cbuf[at].astype(f32)
        inv = inverse_norm(block)
        inv_c[at] = jnp.broadcast_to(inv, (rows, lanes))
        clow[at] = (block * inv).astype(bf16)

    repeat(blocks, normalise, unroll)
    spread_relay(0, emb)

    def send_features(base, first, last):
        def one(i):
            dst = base + lax.rem(me + i, half)
            send(20, fsend.at[dst], frecv.at[me], dst)

        loop(first, last, one)

    first_part = 5 * half // 8
    send_features(far, 0, first_part)

    def hits(at, first):
        ids = lax.broadcasted_iota(jnp.int32, (group, lanes), 1) + first
        return ids == lab[at]

    def find_targets(g):
        at = ds(g, group)

        def block(k):
            chosen = [
                jnp.where(hits(at, k * rows + j * lanes), 1.0, 0.0).astype(bf16)
                for j in range(rows // lanes)
            ]
            acc[at] += jnp.dot(
                jnp.concatenate(chosen, axis=1), clow[ds(k, rows)], preferred_element_type=f32
            )

        acc[at] = jnp.zeros((group, width), f32)
        repeat(blocks, block, unroll)
        target[ds(g, group // tok)] = acc[at].astype(bf16).reshape(group // tok, tok, width)

    loop(0, groups, find_targets)
    spread_near(0, emb)
    loop(groups, 2 * groups, find_targets)
    loop(0, half, lambda j: send(7, target.at[2 * j + 1 - core], tpair.at[j], partner))

    def forward(g):
        at = ds(g, group)
        raw = emb[ds(g, group // tok)].reshape(group, width).astype(f32)
        picked = (raw * inverse_norm(raw)).astype(bf16)
        low[at] = picked
        sums[at] = jnp.zeros((group, lanes), f32)

        def block(k):
            cos = lax.dot_general(
                picked, clow[ds(k, rows)], (((1,), (1,)), ((), ())), preferred_element_type=f32
            )
            row = jnp.zeros((group, lanes), f32)
            for j in range(rows // lanes):
                power = jnp.exp2(exp2_scale * cos[:, j * lanes : (j + 1) * lanes])
                power = jnp.where(hits(at, k * rows + j * lanes), 0.0, power)
                row = row + power
                expo[at, ds(k * (rows // lanes) + j, lanes)] = power.astype(bf16)
            sums[at] += row

        repeat(blocks, block, unroll)

    def weigh(g):
        at = ds(g, 256)
        acc[at] = jnp.dot(expo[at], clow[...], preferred_element_type=f32)
        psend[ds(g, 256 // tok)] = acc[at].astype(bf16).reshape(256 // tok, tok, width)

    def each_group(base, size, body):
        count = batch // 2 // size
        if count == 1:
            body(base)
        else:
            loop(0, count, lambda g: body(base * count + g))

    def add_target(j):
        mine = target[2 * j + core].astype(f32)
        blocks_t[j] = (mine + tpair[j].astype(f32)).astype(bf16)

    def send_pair(phase, first):
        def one(j):
            send(phase, psend.at[2 * (first + j) + 1 - core], pair.at[first + j], partner)

        loop(0, quarter, one)

    def add_pair(first):
        def one(j):
            to = first + j
            at = pl.ds(pl.multiple_of((2 * to + core) * tok, tok), tok)
            blocks_u[to] = (acc[at] + pair[to].astype(f32)).astype(bf16)

        loop(0, quarter, one)

    near_chips, far_chips = side * quarter, (1 - side) * quarter
    wait_all(rsems, 3, emb, quarter)
    each_group(side, group, forward)
    wait_all(rsems, 7, tpair, half)
    loop(0, half, add_target)
    fold_far(8, blocks_t, far_t)
    fold_near(9, blocks_t, near_t)
    spread_far(0, emb)
    send_features(far, first_part, half)
    each_group(side, 256, weigh)
    send_pair(21, near_chips)
    wait_all(rsems, 4, emb, quarter)
    each_group(1 - side, group, forward)
    wait_all(rsems, 21, pair, quarter)
    add_pair(near_chips)
    fold_near(13, blocks_u, near_u)
    each_group(1 - side, 256, weigh)
    send_pair(11, far_chips)

    mine = (local >= 0) & (local < classes)
    picked = target[...].reshape(batch, width).astype(f32)
    tcos = row_sums(low[...].astype(f32) * picked)
    tsin = jnp.sqrt(1.0 - tcos * tcos)
    texp = jnp.exp(logit_scale * (tcos * cos_margin - tsin * sin_margin))
    slope = cos_margin + sin_margin * tcos / tsin
    ssend[...] = row_sums(sums[...]) + jnp.where(mine, texp, 0.0)
    srecv[me] = ssend[...]

    def send_stats(i):
        to = lax.rem(me + i, n)
        send(22, ssend, srecv.at[me], to)

    wait_all(rsems, 11, pair, quarter)
    add_pair(far_chips)
    fold_far(12, blocks_u, far_u)
    fold_cross(8, far_t, 0)
    loop(1, n, send_stats)
    own = esend[...].astype(f32)
    inv_emb = inverse_norm(own)
    emb_dir = own * inv_emb
    fold_cross(12, far_u, 1)

    wait_all(rsems, 22, srecv, n - 1)
    norm = jnp.sum(srecv[...], axis=0)
    scale = column(logit_scale / norm)
    tfix[...] = column((texp - norm) * slope)
    for j in range(width // lanes):
        at = slice(j * lanes, (j + 1) * lanes)
        low[:, at] = (low[:, at].astype(f32) * scale).astype(bf16)

    ones = jnp.ones((width, lanes), bf16)

    def center_grads(k):
        at = ds(k, rows)
        weights = []
        for j in range(rows // lanes):
            block = expo[:, ds(k * (rows // lanes) + j, lanes)].astype(f32)
            ids = lax.broadcasted_iota(jnp.int32, (batch, lanes), 1) + (k * rows + j * lanes)
            weights.append(jnp.where(ids == lab[...], tfix[...], block).astype(bf16))
        unit = lax.dot_general(
            jnp.concatenate(weights, axis=1), low[...], (((0,), (0,)), ((), ())),
            preferred_element_type=f32,
        )
        center = cbuf[at].astype(f32)
        along = jnp.dot((unit * center).astype(bf16), ones, preferred_element_type=f32)
        inv = inv_c[at]
        along = along * (inv * inv * inv)
        for j in range(width // lanes):
            cols = slice(j * lanes, (j + 1) * lanes)
            gc_out[at, cols] = (unit[:, cols] * inv - center[:, cols] * along).astype(bf16)

    stops = [blocks * i // 16 for i in (0, 3, 8, 13, 16)]
    loop(stops[0], stops[1], center_grads)
    own_target = fold_end(8, near_t, 0)
    own_low = emb_dir.astype(bf16).astype(f32)
    own_cos = jnp.sum(own_low * own_target, axis=1, keepdims=True)
    own_sin = jnp.sqrt(1.0 - own_cos * own_cos)
    own_logit = logit_scale * (own_cos * cos_margin - own_sin * sin_margin)
    own_slope = cos_margin + sin_margin * own_cos / own_sin
    own_row = lax.broadcasted_iota(jnp.int32, (tok, batch), 0) + me * tok
    own_lane = lax.broadcasted_iota(jnp.int32, (tok, batch), 1)
    own_norm = jnp.sum(jnp.where(own_row == own_lane, norm, 0.0), axis=1, keepdims=True)
    loss = jnp.log(own_norm) - own_logit
    loss_out[...] = jnp.broadcast_to(loss, (tok, lanes)).T[0:1]
    own_scale = logit_scale / own_norm
    own_grad = logit_scale * (jnp.exp(own_logit) / own_norm - 1.0) * own_slope
    grad_dir = own_scale * fold_end(12, near_u, 1) + own_grad * own_target
    along = jnp.sum(grad_dir * emb_dir, axis=1, keepdims=True)
    grad_emb = ((grad_dir - emb_dir * along) * inv_emb).astype(bf16)
    gsend[...] = grad_emb
    grecv[me] = grad_emb
    spread_start(15, gsend, grecv)
    loop(stops[1], stops[2], center_grads)
    spread_relay(15, grecv)
    send_features(near, 1, half)
    loop(stops[2], stops[3], center_grads)
    spread_near(15, grecv)
    loop(stops[3], stops[4], center_grads)
    spread_far(15, grecv)
    wait_all(rsems, 20, frecv, n - 1)
    wait_all(ssems, 20, frecv, n - 1)
    wait_all(ssems, 22, srecv, n - 1)
    wait_all(ssems, 7, tpair, half)
    wait_all(ssems, 11, pair, quarter)
    wait_all(ssems, 21, pair, quarter)
    spread_end(0, emb)
    wait_all(rsems, 18, grecv, quarter)
    wait_all(rsems, 19, grecv, quarter)
    spread_end(15, grecv)


def last_kernel(gc, features, grads, loss, loss_out, gc_out, fc_out, stage, sems):
    classes = gc.shape[0]
    pieces = 16
    for i in range(pieces):
        at = pl.ds(i * (classes // pieces), classes // pieces)
        pltpu.make_async_copy(gc.at[at], gc_out.at[at], sems.at[0]).start()
    n, tok, part = features.shape
    stage[...] = lax.dot_general(
        features[...].reshape(n * tok, part), grads[...].reshape(n * tok, grads.shape[2]),
        (((0,), (0,)), ((), ())), preferred_element_type=f32,
    )
    fc_copy = pltpu.make_async_copy(stage, fc_out, sems.at[1])
    fc_copy.start()
    loss_out[...] = loss[0]
    pltpu.make_async_copy(gc, gc_out, sems.at[0]).wait()
    fc_copy.wait()


def on_device(features, fc_weight, centers, labels):
    n = lax.axis_size("cls")
    tok, feats = features.shape
    classes, width = centers.shape
    batch = labels.shape[0]
    rows = 256
    chunk = lanes * largest_divisor(feats // lanes, 14)
    split = largest_divisor(chunk // lanes, 7)
    slots = feats // chunk if batch <= 1024 else 2
    part = feats // n
    vmem = pl.BlockSpec(memory_space=pltpu.VMEM)
    hbm = pl.BlockSpec(memory_space=pl.ANY)
    loss, gc, spread, grads = pl.pallas_call(
        functools.partial(main_kernel, n, rows, slots, split),
        out_shape=(
            pltpu.VMEM((1, tok), f32),
            pltpu.VMEM((classes, width), bf16),
            pltpu.VMEM((n, tok, part), bf16),
            pltpu.VMEM((n, tok, width), bf16),
        ),
        in_specs=[hbm, hbm, hbm, vmem],
        out_specs=(vmem, vmem, vmem, vmem),
        scratch_shapes=[
            pltpu.VMEM((tok, feats), bf16),
            pltpu.VMEM((slots, chunk, width), bf16),
            pltpu.VMEM((classes, width), bf16),
            pltpu.VMEM((classes, width), bf16),
            pltpu.VMEM((classes, lanes), f32),
            pltpu.VMEM((batch, classes), bf16),
            pltpu.VMEM((batch, lanes), f32),
            pltpu.VMEM((batch, width), f32),
            pltpu.VMEM((n, tok, width), bf16),
            pltpu.VMEM((tok, width), bf16),
            pltpu.VMEM((n, tok, width), bf16),
            pltpu.VMEM((batch, width), bf16),
            pltpu.VMEM((batch, lanes), jnp.int32),
            pltpu.VMEM((batch, lanes), f32),
            pltpu.VMEM((n, tok, part), bf16),
            pltpu.VMEM((1, batch), f32),
            pltpu.VMEM((n, 1, batch), f32),
            pltpu.VMEM((n, tok, width), bf16),
            pltpu.VMEM((n // 2, tok, width), bf16),
            pltpu.VMEM((n // 2, tok, width), bf16),
            pltpu.VMEM((n // 2, tok, width), bf16),
            pltpu.VMEM((n // 2, tok, width), bf16),
            pltpu.VMEM((n // 4, tok, width), bf16),
            pltpu.VMEM((n // 4, tok, width), bf16),
            pltpu.VMEM((n // 4, tok, width), bf16),
            pltpu.VMEM((n // 4, tok, width), bf16),
            pltpu.VMEM((2, tok, width), bf16),
            pltpu.VMEM((2, tok, width), bf16),
            pltpu.VMEM((tok, width), bf16),
            pltpu.SemaphoreType.DMA((feats // chunk,)),
            pltpu.SemaphoreType.DMA((slots,)),
            pltpu.SemaphoreType.DMA,
            pltpu.SemaphoreType.DMA((23,)),
            pltpu.SemaphoreType.DMA((23,)),
        ],
        compiler_params=pltpu.CompilerParams(
            collective_id=0, has_side_effects=True, vmem_limit_bytes=57 * 2**20
        ),
    )(features, fc_weight, centers, labels[None])
    return pl.pallas_call(
        last_kernel,
        out_shape=(
            jax.ShapeDtypeStruct((tok,), f32),
            jax.ShapeDtypeStruct((classes, width), bf16),
            jax.ShapeDtypeStruct((part, width), f32),
        ),
        in_specs=[vmem, vmem, vmem, vmem],
        out_specs=(vmem, hbm, hbm),
        scratch_shapes=[pltpu.VMEM((part, width), f32), pltpu.SemaphoreType.DMA((2,))],
        compiler_params=pltpu.CompilerParams(vmem_limit_bytes=8 * 2**20),
    )(gc, spread, grads, loss)


def solution(mesh):
    placed = (P("cls", None), P(), P("cls", None), P())
    return jax.shard_map(
        on_device,
        mesh=mesh,
        in_specs=placed,
        out_specs=(P("cls"), P("cls", None), P("cls", None)),
        check_vma=False,
    )
```

```python
import functools
import math

import jax
import jax.numpy as jnp
from jax import lax
from jax.experimental import pallas as pl
from jax.experimental.pallas import tpu as pltpu
from jax.sharding import PartitionSpec as P

logit_scale = 64.0
cos_margin = math.cos(0.5)
sin_margin = math.sin(0.5)
epsilon = 1e-06
exp2_scale = logit_scale * math.log2(math.e)
lanes = 128
MESH = pl.DeviceIdType.MESH
f32, bf16 = jnp.float32, jnp.bfloat16


def inverse_norm(values):
    return lax.rsqrt(jnp.sum(values * values, axis=1, keepdims=True) + epsilon)


def largest_divisor(number, most):
    return next(d for d in range(most, 0, -1) if number % d == 0)


def repeat(count, body, unroll):
    if unroll:
        for k in range(count):
            body(k)
    else:
        lax.fori_loop(0, count, lambda k, carry: (body(k), carry)[1], 0)


def ds(k, size):
    return pl.ds(k * size if isinstance(k, int) else pl.multiple_of(k * size, size), size)


def row_sums(values):
    part = values[:, :lanes]
    for j in range(1, values.shape[1] // lanes):
        part = part + values[:, j * lanes : (j + 1) * lanes]
    return jnp.sum(part.T, axis=0, keepdims=True)


def column(row):
    return jnp.broadcast_to(row, (lanes, row.shape[1])).T


def main_kernel(
    n, rows, slots, split, feat_hbm, weight, centers_hbm, labels,
    loss_out, gc_out, features_out, grads_out,
    feat, wbuf, cbuf, clow, inv_c, expo, sums, acc, target, esend, emb, low,
    lab, tfix, fsend, ssend, srecv, psend, pair, tpair, blocks_u, blocks_t,
    far_u, across_u, near_u, far_t, near_t, fold_send, fold_recv, gsend,
    fsem, wsem, csem, ssems, rsems,
):
    me = lax.axis_index("cls")
    tok, feats = feat.shape
    classes, width = cbuf.shape
    batch = n * tok
    chunk = wbuf.shape[1]
    chunks = feats // chunk
    blocks = classes // rows
    part = feats // n
    half = n // 2
    quarter = n // 4
    core = lax.rem(me, 2)
    chip = me // 2
    partner = me + 1 - 2 * core
    mirror = lax.rem(me + half, n)
    side = me // half
    near, far = side * half, (1 - side) * half
    place = chip - side * quarter
    eighth = n // 8
    plane = place // eighth
    spot = place - plane * eighth
    unroll = batch <= 512
    group = min(batch // 2, 512)
    groups = batch // 2 // group
    frecv, grecv = features_out, grads_out

    def feat_copy(c):
        at = pl.ds(c * chunk, chunk)
        return pltpu.make_async_copy(feat_hbm.at[:, at], feat.at[:, at], fsem.at[c])

    def weight_start(c):
        size = chunk // split
        for i in range(split):
            pltpu.make_async_copy(
                weight.at[pl.ds(c * chunk + i * size, size)],
                wbuf.at[c % slots, pl.ds(i * size, size)],
                wsem.at[c % slots],
            ).start()

    def weight_wait(c):
        pltpu.make_async_copy(
            weight.at[pl.ds(c * chunk, chunk)], wbuf.at[c % slots], wsem.at[c % slots]
        ).wait()

    barrier = pltpu.get_barrier_semaphore()

    def greet(i, carry):
        pl.semaphore_signal(barrier, inc=1, device_id=(lax.rem(me + i, n),), device_id_type=MESH)
        return carry

    ahead = 4 if slots == chunks else slots
    feat_copy(0).start()
    weight_start(0)
    lax.fori_loop(1, n, greet, 0)
    for c in range(1, chunks):
        feat_copy(c).start()
        if c < ahead:
            weight_start(c)

    def send(phase, source, target_ref, to):
        pltpu.make_async_remote_copy(
            src_ref=source, dst_ref=target_ref,
            send_sem=ssems.at[phase], recv_sem=rsems.at[phase],
            device_id=(to,), device_id_type=MESH,
        ).start()

    def loop(first, last, body):
        lax.fori_loop(first, last, lambda i, carry: (body(i), carry)[1], 0)

    def wait_all(sems, phase, target_ref, count):
        whole = target_ref.at[pl.ds(0, count)]
        pltpu.make_async_copy(whole, whole, sems.at[phase]).wait()

    def mate(i):
        to = lax.rem(place + i, quarter)
        return to, near + 2 * to + core

    def plane_mate(i):
        to = plane * eighth + lax.rem(spot + i, eighth)
        return to, near + 2 * to + core

    def across(i):
        to = (1 - plane) * eighth + lax.rem(spot + i, eighth)
        return to, far + 2 * to + core

    def spread_mirror(phase, own, whole):
        send(phase, own, whole.at[me], mirror)

    def spread_half(phase, own, whole):
        loop(1, quarter, lambda i: send(phase + 1, own, whole.at[me], mate(i)[1]))

    def spread_across(direct, own, whole):
        loop(0, eighth, lambda i: send(direct, own, whole.at[me], across(i)[1]))

    def spread_relay(phase, whole):
        wait_all(rsems, phase, whole, 1)
        block = whole.at[mirror]
        loop(1, eighth, lambda i: send(phase + 2, block, block, plane_mate(i)[1]))

    def spread_near(phase, whole):
        wait_all(rsems, phase + 1, whole, quarter - 1)

        def one(j):
            block = whole.at[near + 2 * j + core]
            send(phase + 3, block, block, partner)

        loop(0, quarter, one)

    def spread_far(phase, direct, whole):
        wait_all(rsems, phase + 2, whole, eighth - 1)
        wait_all(rsems, direct, whole, eighth)

        def one(j):
            block = whole.at[far + 2 * j + core]
            send(phase + 4, block, block, partner)

        loop(0, quarter, one)

    def spread_end(phase, direct, whole):
        for i, count in enumerate((1, quarter - 1, eighth - 1, quarter, quarter)):
            wait_all(ssems, phase + i, whole, count)
        wait_all(ssems, direct, whole, eighth)

    def fold_far(phase, parts, buf):
        def one(i):
            to, device = mate(i)
            send(phase, parts.at[(1 - side) * quarter + to], buf.at[place], device)

        loop(1, quarter, one)
        buf[place] = parts[(1 - side) * quarter + place]

    def fold_plane(phase, direct, parts, buf, direct_buf):
        def one(i):
            to, device = plane_mate(i)
            send(phase, parts.at[(1 - side) * quarter + to], buf.at[spot], device)

        def other(i):
            to, device = across(i)
            send(direct, parts.at[(1 - side) * quarter + to], direct_buf.at[spot], device)

        loop(1, eighth, one)
        loop(0, eighth, other)
        buf[spot] = parts[(1 - side) * quarter + place]

    def fold_near(phase, parts, buf):
        def one(i):
            to, device = mate(i)
            send(phase, parts.at[side * quarter + to], buf.at[place], device)

        loop(1, quarter, one)
        buf[place] = parts[chip]

    def fold_cross(phase, far_buf, which, count):
        wait_all(rsems, phase, far_buf, count - 1)
        fold_send[which] = jnp.sum(far_buf[...].astype(f32), axis=0).astype(bf16)
        send(phase + 2, fold_send.at[which], fold_recv.at[which], mirror)

    def fold_end(phase, near_buf, which, count):
        wait_all(rsems, phase + 1, near_buf, quarter - 1)
        wait_all(rsems, phase + 2, near_buf, 1)
        for i, sent in enumerate((count - 1, quarter - 1, 1)):
            wait_all(ssems, phase + i, near_buf, sent)
        return jnp.sum(near_buf[...].astype(f32), axis=0) + fold_recv[which].astype(f32)

    total = jnp.zeros((tok, width), f32)
    for c in range(chunks):
        feat_copy(c).wait()
        weight_wait(c)
        if slots == chunks and c + ahead < chunks:
            weight_start(c + ahead)
        total = total + jnp.dot(
            feat[:, c * chunk : (c + 1) * chunk], wbuf[c % slots], preferred_element_type=f32
        )
        if slots < chunks and c + ahead < chunks:
            weight_start(c + ahead)
        if c == max(chunks - ahead, 0):
            for i in range(4):
                at = pl.ds(i * (classes // 4), classes // 4)
                pltpu.make_async_copy(centers_hbm.at[at], cbuf.at[at], csem).start()
    esend[...] = total.astype(bf16)
    emb[me] = total.astype(bf16)
    pl.semaphore_wait(barrier, n - 1)
    spread_mirror(0, esend, emb)
    spread_half(0, esend, emb)
    spread_across(23, esend, emb)
    for j in range(n):
        fsend[j] = feat[:, j * part : (j + 1) * part]
    frecv[me] = fsend[me]
    local = labels[...] - me * classes
    lab[...] = column(local.astype(f32)).astype(jnp.int32)

    pltpu.make_async_copy(centers_hbm, cbuf, csem).wait()

    def normalise(k):
        at = ds(k, rows)
        block = cbuf[at].astype(f32)
        inv = inverse_norm(block)
        inv_c[at] = jnp.broadcast_to(inv, (rows, lanes))
        clow[at] = (block * inv).astype(bf16)

    repeat(blocks, normalise, unroll)
    spread_relay(0, emb)

    def send_features(base, first, last):
        def one(i):
            dst = base + lax.rem(me + i, half)
            send(20, fsend.at[dst], frecv.at[me], dst)

        loop(first, last, one)

    first_part, second_part = 10 * half // 16, 13 * half // 16
    send_features(far, 0, first_part)

    def hits(at, first):
        ids = lax.broadcasted_iota(jnp.int32, (group, lanes), 1) + first
        return ids == lab[at]

    def find_targets(g):
        at = ds(g, group)

        def block(k):
            chosen = [
                jnp.where(hits(at, k * rows + j * lanes), 1.0, 0.0).astype(bf16)
                for j in range(rows // lanes)
            ]
            acc[at] += jnp.dot(
                jnp.concatenate(chosen, axis=1), clow[ds(k, rows)], preferred_element_type=f32
            )

        acc[at] = jnp.zeros((group, width), f32)
        repeat(blocks, block, unroll)
        target[ds(g, group // tok)] = acc[at].astype(bf16).reshape(group // tok, tok, width)

    loop(0, groups, find_targets)
    spread_near(0, emb)
    loop(groups, 2 * groups, find_targets)
    loop(0, half, lambda j: send(7, target.at[2 * j + 1 - core], tpair.at[j], partner))

    def forward(g):
        at = ds(g, group)
        raw = emb[ds(g, group // tok)].reshape(group, width).astype(f32)
        picked = (raw * inverse_norm(raw)).astype(bf16)
        low[at] = picked
        sums[at] = jnp.zeros((group, lanes), f32)

        def block(k):
            cos = lax.dot_general(
                picked, clow[ds(k, rows)], (((1,), (1,)), ((), ())), preferred_element_type=f32
            )
            row = jnp.zeros((group, lanes), f32)
            for j in range(rows // lanes):
                power = jnp.exp2(exp2_scale * cos[:, j * lanes : (j + 1) * lanes])
                power = jnp.where(hits(at, k * rows + j * lanes), 0.0, power)
                row = row + power
                expo[at, ds(k * (rows // lanes) + j, lanes)] = power.astype(bf16)
            sums[at] += row

        repeat(blocks, block, unroll)

    def weigh(g):
        at = ds(g, 256)
        acc[at] = jnp.dot(expo[at], clow[...], preferred_element_type=f32)
        psend[ds(g, 256 // tok)] = acc[at].astype(bf16).reshape(256 // tok, tok, width)

    def each_group(base, size, body):
        count = batch // 2 // size
        if count == 1:
            body(base)
        else:
            loop(0, count, lambda g: body(base * count + g))

    def add_target(j):
        mine = target[2 * j + core].astype(f32)
        blocks_t[j] = (mine + tpair[j].astype(f32)).astype(bf16)

    def send_pair(phase, first):
        def one(j):
            send(phase, psend.at[2 * (first + j) + 1 - core], pair.at[first + j], partner)

        loop(0, quarter, one)

    def add_pair(first):
        def one(j):
            to = first + j
            at = pl.ds(pl.multiple_of((2 * to + core) * tok, tok), tok)
            blocks_u[to] = (acc[at] + pair[to].astype(f32)).astype(bf16)

        loop(0, quarter, one)

    near_chips, far_chips = side * quarter, (1 - side) * quarter
    wait_all(rsems, 3, emb, quarter)
    each_group(side, group, forward)
    spread_far(0, 23, emb)
    wait_all(rsems, 7, tpair, half)
    loop(0, half, add_target)
    fold_far(8, blocks_t, far_t)
    fold_near(9, blocks_t, near_t)
    each_group(side, 256, weigh)
    send_pair(21, near_chips)
    wait_all(rsems, 4, emb, quarter)
    each_group(1 - side, group, forward)

    mine = (local >= 0) & (local < classes)
    picked = target[...].reshape(batch, width).astype(f32)
    tcos = row_sums(low[...].astype(f32) * picked)
    tsin = jnp.sqrt(1.0 - tcos * tcos)
    texp = jnp.exp(logit_scale * (tcos * cos_margin - tsin * sin_margin))
    slope = cos_margin + sin_margin * tcos / tsin
    ssend[...] = row_sums(sums[...]) + jnp.where(mine, texp, 0.0)
    srecv[me] = ssend[...]

    def send_stats(i):
        to = lax.rem(me + i, n)
        send(22, ssend, srecv.at[me], to)

    loop(1, n, send_stats)
    each_group(1 - side, 256, weigh)
    send_pair(11, far_chips)
    wait_all(rsems, 21, pair, quarter)
    add_pair(near_chips)
    fold_cross(8, far_t, 0, quarter)
    wait_all(rsems, 11, pair, quarter)
    add_pair(far_chips)
    fold_plane(12, 25, blocks_u, far_u, across_u)
    fold_near(13, blocks_u, near_u)
    own = esend[...].astype(f32)
    inv_emb = inverse_norm(own)
    emb_dir = own * inv_emb
    fold_cross(12, far_u, 1, eighth)
    send_features(far, first_part, second_part)
    send_features(near, 1, half)

    wait_all(rsems, 22, srecv, n - 1)
    norm = jnp.sum(srecv[...], axis=0)
    scale = column(logit_scale / norm)
    tfix[...] = column((texp - norm) * slope)
    for j in range(width // lanes):
        at = slice(j * lanes, (j + 1) * lanes)
        low[:, at] = (low[:, at].astype(f32) * scale).astype(bf16)

    ones = jnp.ones((width, lanes), bf16)

    def center_grads(k):
        at = ds(k, rows)
        weights = []
        for j in range(rows // lanes):
            block = expo[:, ds(k * (rows // lanes) + j, lanes)].astype(f32)
            ids = lax.broadcasted_iota(jnp.int32, (batch, lanes), 1) + (k * rows + j * lanes)
            weights.append(jnp.where(ids == lab[...], tfix[...], block).astype(bf16))
        unit = lax.dot_general(
            jnp.concatenate(weights, axis=1), low[...], (((0,), (0,)), ((), ())),
            preferred_element_type=f32,
        )
        center = cbuf[at].astype(f32)
        along = jnp.dot((unit * center).astype(bf16), ones, preferred_element_type=f32)
        inv = inv_c[at]
        along = along * (inv * inv * inv)
        for j in range(width // lanes):
            cols = slice(j * lanes, (j + 1) * lanes)
            gc_out[at, cols] = (unit[:, cols] * inv - center[:, cols] * along).astype(bf16)

    def grads_between(first, last):
        def two(k):
            center_grads(2 * k)
            center_grads(2 * k + 1)

        loop(blocks // 2 * first // 8, blocks // 2 * last // 8, two)

    grads_between(0, 2)
    own_target = fold_end(8, near_t, 0, quarter)
    own_low = emb_dir.astype(bf16).astype(f32)
    own_cos = jnp.sum(own_low * own_target, axis=1, keepdims=True)
    own_sin = jnp.sqrt(1.0 - own_cos * own_cos)
    own_logit = logit_scale * (own_cos * cos_margin - own_sin * sin_margin)
    own_slope = cos_margin + sin_margin * own_cos / own_sin
    own_row = lax.broadcasted_iota(jnp.int32, (tok, batch), 0) + me * tok
    own_lane = lax.broadcasted_iota(jnp.int32, (tok, batch), 1)
    own_norm = jnp.sum(jnp.where(own_row == own_lane, norm, 0.0), axis=1, keepdims=True)
    loss = jnp.log(own_norm) - own_logit
    loss_out[...] = jnp.broadcast_to(loss, (tok, lanes)).T[0:1]
    own_scale = logit_scale / own_norm
    own_grad = logit_scale * (jnp.exp(own_logit) / own_norm - 1.0) * own_slope
    total = fold_end(12, near_u, 1, eighth)
    wait_all(rsems, 25, across_u, eighth)
    total = total + jnp.sum(across_u[...].astype(f32), axis=0)
    grad_dir = own_scale * total + own_grad * own_target
    along = jnp.sum(grad_dir * emb_dir, axis=1, keepdims=True)
    grad_emb = ((grad_dir - emb_dir * along) * inv_emb).astype(bf16)
    gsend[...] = grad_emb
    grecv[me] = grad_emb
    spread_mirror(15, gsend, grecv)
    spread_across(24, gsend, grecv)
    spread_half(15, gsend, grecv)
    grads_between(2, 5)
    spread_relay(15, grecv)
    send_features(far, second_part, half)
    grads_between(5, 7)
    spread_near(15, grecv)
    spread_far(15, 24, grecv)
    grads_between(7, 8)
    wait_all(rsems, 20, frecv, n - 1)
    wait_all(ssems, 20, frecv, n - 1)
    wait_all(ssems, 22, srecv, n - 1)
    wait_all(ssems, 7, tpair, half)
    wait_all(ssems, 11, pair, quarter)
    wait_all(ssems, 21, pair, quarter)
    wait_all(ssems, 25, across_u, eighth)
    spread_end(0, 23, emb)
    wait_all(rsems, 18, grecv, quarter)
    wait_all(rsems, 19, grecv, quarter)
    spread_end(15, 24, grecv)


def last_kernel(gc, features, grads, loss, loss_out, gc_out, fc_out, stage, sems):
    classes = gc.shape[0]
    pieces = 16
    for i in range(pieces):
        at = pl.ds(i * (classes // pieces), classes // pieces)
        pltpu.make_async_copy(gc.at[at], gc_out.at[at], sems.at[0]).start()
    n, tok, part = features.shape
    stage[...] = lax.dot_general(
        features[...].reshape(n * tok, part), grads[...].reshape(n * tok, grads.shape[2]),
        (((0,), (0,)), ((), ())), preferred_element_type=f32,
    )
    fc_copy = pltpu.make_async_copy(stage, fc_out, sems.at[1])
    fc_copy.start()
    loss_out[...] = loss[0]
    pltpu.make_async_copy(gc, gc_out, sems.at[0]).wait()
    fc_copy.wait()


def on_device(features, fc_weight, centers, labels):
    n = lax.axis_size("cls")
    tok, feats = features.shape
    classes, width = centers.shape
    batch = labels.shape[0]
    rows = 256
    chunk = lanes * largest_divisor(feats // lanes, 14)
    split = largest_divisor(chunk // lanes, 7)
    slots = feats // chunk if batch <= 1024 else 2
    part = feats // n
    vmem = pl.BlockSpec(memory_space=pltpu.VMEM)
    hbm = pl.BlockSpec(memory_space=pl.ANY)
    loss, gc, spread, grads = pl.pallas_call(
        functools.partial(main_kernel, n, rows, slots, split),
        out_shape=(
            pltpu.VMEM((1, tok), f32),
            pltpu.VMEM((classes, width), bf16),
            pltpu.VMEM((n, tok, part), bf16),
            pltpu.VMEM((n, tok, width), bf16),
        ),
        in_specs=[hbm, hbm, hbm, vmem],
        out_specs=(vmem, vmem, vmem, vmem),
        scratch_shapes=[
            pltpu.VMEM((tok, feats), bf16),
            pltpu.VMEM((slots, chunk, width), bf16),
            pltpu.VMEM((classes, width), bf16),
            pltpu.VMEM((classes, width), bf16),
            pltpu.VMEM((classes, lanes), f32),
            pltpu.VMEM((batch, classes), bf16),
            pltpu.VMEM((batch, lanes), f32),
            pltpu.VMEM((batch, width), f32),
            pltpu.VMEM((n, tok, width), bf16),
            pltpu.VMEM((tok, width), bf16),
            pltpu.VMEM((n, tok, width), bf16),
            pltpu.VMEM((batch, width), bf16),
            pltpu.VMEM((batch, lanes), jnp.int32),
            pltpu.VMEM((batch, lanes), f32),
            pltpu.VMEM((n, tok, part), bf16),
            pltpu.VMEM((1, batch), f32),
            pltpu.VMEM((n, 1, batch), f32),
            pltpu.VMEM((n, tok, width), bf16),
            pltpu.VMEM((n // 2, tok, width), bf16),
            pltpu.VMEM((n // 2, tok, width), bf16),
            pltpu.VMEM((n // 2, tok, width), bf16),
            pltpu.VMEM((n // 2, tok, width), bf16),
            pltpu.VMEM((n // 8, tok, width), bf16),
            pltpu.VMEM((n // 8, tok, width), bf16),
            pltpu.VMEM((n // 4, tok, width), bf16),
            pltpu.VMEM((n // 4, tok, width), bf16),
            pltpu.VMEM((n // 4, tok, width), bf16),
            pltpu.VMEM((2, tok, width), bf16),
            pltpu.VMEM((2, tok, width), bf16),
            pltpu.VMEM((tok, width), bf16),
            pltpu.SemaphoreType.DMA((feats // chunk,)),
            pltpu.SemaphoreType.DMA((slots,)),
            pltpu.SemaphoreType.DMA,
            pltpu.SemaphoreType.DMA((26,)),
            pltpu.SemaphoreType.DMA((26,)),
        ],
        compiler_params=pltpu.CompilerParams(
            collective_id=0, has_side_effects=True, vmem_limit_bytes=57 * 2**20
        ),
    )(features, fc_weight, centers, labels[None])
    return pl.pallas_call(
        last_kernel,
        out_shape=(
            jax.ShapeDtypeStruct((tok,), f32),
            jax.ShapeDtypeStruct((classes, width), bf16),
            jax.ShapeDtypeStruct((part, width), f32),
        ),
        in_specs=[vmem, vmem, vmem, vmem],
        out_specs=(vmem, hbm, hbm),
        scratch_shapes=[pltpu.VMEM((part, width), f32), pltpu.SemaphoreType.DMA((2,))],
        compiler_params=pltpu.CompilerParams(vmem_limit_bytes=8 * 2**20),
    )(gc, spread, grads, loss)


def solution(mesh):
    placed = (P("cls", None), P(), P("cls", None), P())
    return jax.shard_map(
        on_device,
        mesh=mesh,
        in_specs=placed,
        out_specs=(P("cls"), P("cls", None), P("cls", None)),
        check_vma=False,
    )
```

```python
import functools
import math

import jax
import jax.numpy as jnp
from jax import lax
from jax.experimental import pallas as pl
from jax.experimental.pallas import tpu as pltpu
from jax.sharding import PartitionSpec as P

logit_scale = 64.0
cos_margin = math.cos(0.5)
sin_margin = math.sin(0.5)
epsilon = 1e-06
exp2_scale = logit_scale * math.log2(math.e)
lanes = 128
MESH = pl.DeviceIdType.MESH
f32, bf16 = jnp.float32, jnp.bfloat16


def inverse_norm(values):
    return lax.rsqrt(jnp.sum(values * values, axis=1, keepdims=True) + epsilon)


def largest_divisor(number, most):
    return next(d for d in range(most, 0, -1) if number % d == 0)


def repeat(count, body, unroll):
    if unroll:
        for k in range(count):
            body(k)
    else:
        lax.fori_loop(0, count, lambda k, carry: (body(k), carry)[1], 0)


def ds(k, size):
    return pl.ds(k * size if isinstance(k, int) else pl.multiple_of(k * size, size), size)


def row_sums(values):
    part = values[:, :lanes]
    for j in range(1, values.shape[1] // lanes):
        part = part + values[:, j * lanes : (j + 1) * lanes]
    return jnp.sum(part.T, axis=0, keepdims=True)


def column(row):
    return jnp.broadcast_to(row, (lanes, row.shape[1])).T


def main_kernel(
    n, rows, slots, split, feat_hbm, weight, centers_hbm, labels,
    loss_out, gc_out, features_out, grads_out,
    feat, wbuf, cbuf, clow, inv_c, expo, sums, acc, target, esend, emb, low,
    lab, tfix, fsend, ssend, srecv, psend, pair, tpair, blocks_u, blocks_t,
    far_u, across_u, near_u, far_t, near_t, fold_send, fold_recv, gsend,
    fsem, wsem, csem, ssems, rsems,
):
    me = lax.axis_index("cls")
    tok, feats = feat.shape
    classes, width = cbuf.shape
    batch = n * tok
    chunk = wbuf.shape[1]
    chunks = feats // chunk
    blocks = classes // rows
    part = feats // n
    half = n // 2
    quarter = n // 4
    core = lax.rem(me, 2)
    chip = me // 2
    partner = me + 1 - 2 * core
    mirror = lax.rem(me + half, n)
    side = me // half
    near, far = side * half, (1 - side) * half
    place = chip - side * quarter
    eighth = n // 8
    plane = place // eighth
    spot = place - plane * eighth
    unroll = batch <= 512
    group = min(batch // 2, 512)
    groups = batch // 2 // group
    frecv, grecv = features_out, grads_out

    def feat_copy(c):
        at = pl.ds(c * chunk, chunk)
        return pltpu.make_async_copy(feat_hbm.at[:, at], feat.at[:, at], fsem.at[c])

    def weight_start(c):
        size = chunk // split
        for i in range(split):
            pltpu.make_async_copy(
                weight.at[pl.ds(c * chunk + i * size, size)],
                wbuf.at[c % slots, pl.ds(i * size, size)],
                wsem.at[c % slots],
            ).start()

    def weight_wait(c):
        pltpu.make_async_copy(
            weight.at[pl.ds(c * chunk, chunk)], wbuf.at[c % slots], wsem.at[c % slots]
        ).wait()

    barrier = pltpu.get_barrier_semaphore()

    def greet(i, carry):
        pl.semaphore_signal(barrier, inc=1, device_id=(lax.rem(me + i, n),), device_id_type=MESH)
        return carry

    ahead = 4 if slots == chunks else slots
    feat_copy(0).start()
    weight_start(0)
    lax.fori_loop(1, n, greet, 0)
    for c in range(1, chunks):
        feat_copy(c).start()
        if c < ahead:
            weight_start(c)

    def send(phase, source, target_ref, to):
        pltpu.make_async_remote_copy(
            src_ref=source, dst_ref=target_ref,
            send_sem=ssems.at[phase], recv_sem=rsems.at[phase],
            device_id=(to,), device_id_type=MESH,
        ).start()

    def loop(first, last, body):
        lax.fori_loop(first, last, lambda i, carry: (body(i), carry)[1], 0)

    def wait_all(sems, phase, target_ref, count):
        whole = target_ref.at[pl.ds(0, count)]
        pltpu.make_async_copy(whole, whole, sems.at[phase]).wait()

    def mate(i):
        to = lax.rem(place + i, quarter)
        return to, near + 2 * to + core

    def plane_mate(i):
        to = plane * eighth + lax.rem(spot + i, eighth)
        return to, near + 2 * to + core

    def across(i):
        to = (1 - plane) * eighth + lax.rem(spot + i, eighth)
        return to, far + 2 * to + core

    def spread_mirror(phase, own, whole):
        send(phase, own, whole.at[me], mirror)

    def spread_half(phase, own, whole):
        loop(1, quarter, lambda i: send(phase + 1, own, whole.at[me], mate(i)[1]))

    def spread_across(direct, own, whole):
        loop(0, eighth, lambda i: send(direct, own, whole.at[me], across(i)[1]))

    def spread_relay(phase, whole):
        wait_all(rsems, phase, whole, 1)
        block = whole.at[mirror]
        loop(1, eighth, lambda i: send(phase + 2, block, block, plane_mate(i)[1]))

    def spread_near(phase, whole):
        wait_all(rsems, phase + 1, whole, quarter - 1)

        def one(j):
            block = whole.at[near + 2 * j + core]
            send(phase + 3, block, block, partner)

        loop(0, quarter, one)

    def spread_far(phase, direct, whole):
        wait_all(rsems, phase + 2, whole, eighth - 1)
        wait_all(rsems, direct, whole, eighth)

        def one(j):
            block = whole.at[far + 2 * j + core]
            send(phase + 4, block, block, partner)

        loop(0, quarter, one)

    def spread_end(phase, direct, whole):
        for i, count in enumerate((1, quarter - 1, eighth - 1, quarter, quarter)):
            wait_all(ssems, phase + i, whole, count)
        wait_all(ssems, direct, whole, eighth)

    def fold_far(phase, parts, buf):
        def one(i):
            to, device = mate(i)
            send(phase, parts.at[(1 - side) * quarter + to], buf.at[place], device)

        loop(1, quarter, one)
        buf[place] = parts[(1 - side) * quarter + place]

    def fold_plane(phase, direct, parts, buf, direct_buf):
        def one(i):
            to, device = plane_mate(i)
            send(phase, parts.at[(1 - side) * quarter + to], buf.at[spot], device)

        def other(i):
            to, device = across(i)
            send(direct, parts.at[(1 - side) * quarter + to], direct_buf.at[spot], device)

        loop(1, eighth, one)
        loop(0, eighth, other)
        buf[spot] = parts[(1 - side) * quarter + place]

    def fold_near(phase, parts, buf):
        def one(i):
            to, device = mate(i)
            send(phase, parts.at[side * quarter + to], buf.at[place], device)

        loop(1, quarter, one)
        buf[place] = parts[chip]

    def fold_cross(phase, far_buf, which, count):
        wait_all(rsems, phase, far_buf, count - 1)
        fold_send[which] = jnp.sum(far_buf[...].astype(f32), axis=0).astype(bf16)
        send(phase + 2, fold_send.at[which], fold_recv.at[which], mirror)

    def fold_end(phase, near_buf, which, count):
        wait_all(rsems, phase + 1, near_buf, quarter - 1)
        wait_all(rsems, phase + 2, near_buf, 1)
        for i, sent in enumerate((count - 1, quarter - 1, 1)):
            wait_all(ssems, phase + i, near_buf, sent)
        return jnp.sum(near_buf[...].astype(f32), axis=0) + fold_recv[which].astype(f32)

    total = jnp.zeros((tok, width), f32)
    for c in range(chunks):
        feat_copy(c).wait()
        weight_wait(c)
        if slots == chunks and c + ahead < chunks:
            weight_start(c + ahead)
        total = total + jnp.dot(
            feat[:, c * chunk : (c + 1) * chunk], wbuf[c % slots], preferred_element_type=f32
        )
        if slots < chunks and c + ahead < chunks:
            weight_start(c + ahead)
        if c == max(chunks - ahead, 0):
            for i in range(4):
                at = pl.ds(i * (classes // 4), classes // 4)
                pltpu.make_async_copy(centers_hbm.at[at], cbuf.at[at], csem).start()
    esend[...] = total.astype(bf16)
    emb[me] = total.astype(bf16)
    pl.semaphore_wait(barrier, n - 1)
    spread_mirror(0, esend, emb)
    spread_half(0, esend, emb)
    spread_across(23, esend, emb)
    for j in range(n):
        fsend[j] = feat[:, j * part : (j + 1) * part]
    frecv[me] = fsend[me]
    local = labels[...] - me * classes
    lab[...] = column(local.astype(f32)).astype(jnp.int32)

    pltpu.make_async_copy(centers_hbm, cbuf, csem).wait()

    def normalise(k):
        at = ds(k, rows)
        block = cbuf[at].astype(f32)
        inv = inverse_norm(block)
        inv_c[at] = jnp.broadcast_to(inv, (rows, lanes))
        clow[at] = (block * inv).astype(bf16)

    repeat(blocks, normalise, unroll)
    spread_relay(0, emb)

    def send_features(base, first, last):
        def one(i):
            dst = base + lax.rem(me + i, half)
            send(20, fsend.at[dst], frecv.at[me], dst)

        loop(first, last, one)

    first_part = 14 * half // 16
    send_features(far, 0, first_part)

    def hits(at, first):
        ids = lax.broadcasted_iota(jnp.int32, (group, lanes), 1) + first
        return ids == lab[at]

    def find_targets(g):
        at = ds(g, group)

        def block(k):
            chosen = [
                jnp.where(hits(at, k * rows + j * lanes), 1.0, 0.0).astype(bf16)
                for j in range(rows // lanes)
            ]
            acc[at] += jnp.dot(
                jnp.concatenate(chosen, axis=1), clow[ds(k, rows)], preferred_element_type=f32
            )

        acc[at] = jnp.zeros((group, width), f32)
        repeat(blocks, block, unroll)
        target[ds(g, group // tok)] = acc[at].astype(bf16).reshape(group // tok, tok, width)

    loop(0, groups, find_targets)
    spread_near(0, emb)
    loop(groups, 2 * groups, find_targets)
    loop(0, half, lambda j: send(7, target.at[2 * j + 1 - core], tpair.at[j], partner))

    def forward(g):
        at = ds(g, group)
        raw = emb[ds(g, group // tok)].reshape(group, width).astype(f32)
        picked = (raw * inverse_norm(raw)).astype(bf16)
        low[at] = picked
        sums[at] = jnp.zeros((group, lanes), f32)

        def block(k):
            cos = lax.dot_general(
                picked, clow[ds(k, rows)], (((1,), (1,)), ((), ())), preferred_element_type=f32
            )
            row = jnp.zeros((group, lanes), f32)
            for j in range(rows // lanes):
                power = jnp.exp2(exp2_scale * cos[:, j * lanes : (j + 1) * lanes])
                power = jnp.where(hits(at, k * rows + j * lanes), 0.0, power)
                row = row + power
                expo[at, ds(k * (rows // lanes) + j, lanes)] = power.astype(bf16)
            sums[at] += row

        repeat(blocks, block, unroll)

    def weigh(g):
        at = ds(g, 256)
        acc[at] = jnp.dot(expo[at], clow[...], preferred_element_type=f32)
        psend[ds(g, 256 // tok)] = acc[at].astype(bf16).reshape(256 // tok, tok, width)

    def each_group(base, size, body):
        count = batch // 2 // size
        if count == 1:
            body(base)
        else:
            loop(0, count, lambda g: body(base * count + g))

    def add_target(j):
        mine = target[2 * j + core].astype(f32)
        blocks_t[j] = (mine + tpair[j].astype(f32)).astype(bf16)

    def send_pair(phase, first):
        def one(j):
            send(phase, psend.at[2 * (first + j) + 1 - core], pair.at[first + j], partner)

        loop(0, quarter, one)

    def add_pair(first):
        def one(j):
            to = first + j
            at = pl.ds(pl.multiple_of((2 * to + core) * tok, tok), tok)
            blocks_u[to] = (acc[at] + pair[to].astype(f32)).astype(bf16)

        loop(0, quarter, one)

    near_chips, far_chips = side * quarter, (1 - side) * quarter
    wait_all(rsems, 3, emb, quarter)
    each_group(side, group, forward)
    spread_far(0, 23, emb)
    wait_all(rsems, 7, tpair, half)
    loop(0, half, add_target)
    fold_far(8, blocks_t, far_t)
    fold_near(9, blocks_t, near_t)
    each_group(side, 256, weigh)
    send_pair(21, near_chips)
    wait_all(rsems, 4, emb, quarter)
    each_group(1 - side, group, forward)
    each_group(1 - side, 256, weigh)
    send_pair(11, far_chips)

    mine = (local >= 0) & (local < classes)
    picked = target[...].reshape(batch, width).astype(f32)
    tcos = row_sums(low[...].astype(f32) * picked)
    tsin = jnp.sqrt(1.0 - tcos * tcos)
    texp = jnp.exp(logit_scale * (tcos * cos_margin - tsin * sin_margin))
    slope = cos_margin + sin_margin * tcos / tsin
    ssend[...] = row_sums(sums[...]) + jnp.where(mine, texp, 0.0)
    srecv[me] = ssend[...]

    def send_stats(i):
        to = lax.rem(me + i, n)
        send(22, ssend, srecv.at[me], to)

    loop(1, n, send_stats)
    wait_all(rsems, 21, pair, quarter)
    add_pair(near_chips)
    fold_cross(8, far_t, 0, quarter)
    wait_all(rsems, 11, pair, quarter)
    add_pair(far_chips)
    fold_plane(12, 25, blocks_u, far_u, across_u)
    fold_near(13, blocks_u, near_u)
    own = esend[...].astype(f32)
    inv_emb = inverse_norm(own)
    emb_dir = own * inv_emb
    fold_cross(12, far_u, 1, eighth)
    send_features(far, first_part, half)
    send_features(near, 1, half)

    wait_all(rsems, 22, srecv, n - 1)
    norm = jnp.sum(srecv[...], axis=0)
    scale = column(logit_scale / norm)
    tfix[...] = column((texp - norm) * slope)
    for j in range(width // lanes):
        at = slice(j * lanes, (j + 1) * lanes)
        low[:, at] = (low[:, at].astype(f32) * scale).astype(bf16)

    ones = jnp.ones((width, lanes), bf16)

    def center_grads(k):
        at = ds(k, rows)
        weights = []
        for j in range(rows // lanes):
            block = expo[:, ds(k * (rows // lanes) + j, lanes)].astype(f32)
            ids = lax.broadcasted_iota(jnp.int32, (batch, lanes), 1) + (k * rows + j * lanes)
            weights.append(jnp.where(ids == lab[...], tfix[...], block).astype(bf16))
        unit = lax.dot_general(
            jnp.concatenate(weights, axis=1), low[...], (((0,), (0,)), ((), ())),
            preferred_element_type=f32,
        )
        center = cbuf[at].astype(f32)
        along = jnp.dot((unit * center).astype(bf16), ones, preferred_element_type=f32)
        inv = inv_c[at]
        along = along * (inv * inv * inv)
        for j in range(width // lanes):
            cols = slice(j * lanes, (j + 1) * lanes)
            gc_out[at, cols] = (unit[:, cols] * inv - center[:, cols] * along).astype(bf16)

    def grads_between(first, last):
        def two(k):
            center_grads(2 * k)
            center_grads(2 * k + 1)

        loop(blocks // 2 * first // 8, blocks // 2 * last // 8, two)

    grads_between(0, 1)
    own_target = fold_end(8, near_t, 0, quarter)
    own_low = emb_dir.astype(bf16).astype(f32)
    own_cos = jnp.sum(own_low * own_target, axis=1, keepdims=True)
    own_sin = jnp.sqrt(1.0 - own_cos * own_cos)
    own_logit = logit_scale * (own_cos * cos_margin - own_sin * sin_margin)
    own_slope = cos_margin + sin_margin * own_cos / own_sin
    own_row = lax.broadcasted_iota(jnp.int32, (tok, batch), 0) + me * tok
    own_lane = lax.broadcasted_iota(jnp.int32, (tok, batch), 1)
    own_norm = jnp.sum(jnp.where(own_row == own_lane, norm, 0.0), axis=1, keepdims=True)
    loss = jnp.log(own_norm) - own_logit
    loss_out[...] = jnp.broadcast_to(loss, (tok, lanes)).T[0:1]
    own_scale = logit_scale / own_norm
    own_grad = logit_scale * (jnp.exp(own_logit) / own_norm - 1.0) * own_slope
    total = fold_end(12, near_u, 1, eighth)
    wait_all(rsems, 25, across_u, eighth)
    total = total + jnp.sum(across_u[...].astype(f32), axis=0)
    grad_dir = own_scale * total + own_grad * own_target
    along = jnp.sum(grad_dir * emb_dir, axis=1, keepdims=True)
    grad_emb = ((grad_dir - emb_dir * along) * inv_emb).astype(bf16)
    gsend[...] = grad_emb
    grecv[me] = grad_emb
    spread_mirror(15, gsend, grecv)
    spread_across(24, gsend, grecv)
    spread_half(15, gsend, grecv)
    grads_between(1, 4)
    spread_relay(15, grecv)
    grads_between(4, 7)
    spread_near(15, grecv)
    spread_far(15, 24, grecv)
    grads_between(7, 8)
    wait_all(rsems, 20, frecv, n - 1)
    wait_all(ssems, 20, frecv, n - 1)
    wait_all(ssems, 22, srecv, n - 1)
    wait_all(ssems, 7, tpair, half)
    wait_all(ssems, 11, pair, quarter)
    wait_all(ssems, 21, pair, quarter)
    wait_all(ssems, 25, across_u, eighth)
    spread_end(0, 23, emb)
    wait_all(rsems, 18, grecv, quarter)
    wait_all(rsems, 19, grecv, quarter)
    spread_end(15, 24, grecv)


def last_kernel(gc, features, grads, loss, loss_out, gc_out, fc_out, stage, sems):
    classes = gc.shape[0]
    pieces = 16
    for i in range(pieces):
        at = pl.ds(i * (classes // pieces), classes // pieces)
        pltpu.make_async_copy(gc.at[at], gc_out.at[at], sems.at[0]).start()
    n, tok, part = features.shape
    stage[...] = lax.dot_general(
        features[...].reshape(n * tok, part), grads[...].reshape(n * tok, grads.shape[2]),
        (((0,), (0,)), ((), ())), preferred_element_type=f32,
    )
    fc_copy = pltpu.make_async_copy(stage, fc_out, sems.at[1])
    fc_copy.start()
    loss_out[...] = loss[0]
    pltpu.make_async_copy(gc, gc_out, sems.at[0]).wait()
    fc_copy.wait()


def on_device(features, fc_weight, centers, labels):
    n = lax.axis_size("cls")
    tok, feats = features.shape
    classes, width = centers.shape
    batch = labels.shape[0]
    rows = 256
    chunk = lanes * largest_divisor(feats // lanes, 14)
    split = largest_divisor(chunk // lanes, 7)
    slots = feats // chunk if batch <= 1024 else 2
    part = feats // n
    vmem = pl.BlockSpec(memory_space=pltpu.VMEM)
    hbm = pl.BlockSpec(memory_space=pl.ANY)
    loss, gc, spread, grads = pl.pallas_call(
        functools.partial(main_kernel, n, rows, slots, split),
        out_shape=(
            pltpu.VMEM((1, tok), f32),
            pltpu.VMEM((classes, width), bf16),
            pltpu.VMEM((n, tok, part), bf16),
            pltpu.VMEM((n, tok, width), bf16),
        ),
        in_specs=[hbm, hbm, hbm, vmem],
        out_specs=(vmem, vmem, vmem, vmem),
        scratch_shapes=[
            pltpu.VMEM((tok, feats), bf16),
            pltpu.VMEM((slots, chunk, width), bf16),
            pltpu.VMEM((classes, width), bf16),
            pltpu.VMEM((classes, width), bf16),
            pltpu.VMEM((classes, lanes), f32),
            pltpu.VMEM((batch, classes), bf16),
            pltpu.VMEM((batch, lanes), f32),
            pltpu.VMEM((batch, width), f32),
            pltpu.VMEM((n, tok, width), bf16),
            pltpu.VMEM((tok, width), bf16),
            pltpu.VMEM((n, tok, width), bf16),
            pltpu.VMEM((batch, width), bf16),
            pltpu.VMEM((batch, lanes), jnp.int32),
            pltpu.VMEM((batch, lanes), f32),
            pltpu.VMEM((n, tok, part), bf16),
            pltpu.VMEM((1, batch), f32),
            pltpu.VMEM((n, 1, batch), f32),
            pltpu.VMEM((n, tok, width), bf16),
            pltpu.VMEM((n // 2, tok, width), bf16),
            pltpu.VMEM((n // 2, tok, width), bf16),
            pltpu.VMEM((n // 2, tok, width), bf16),
            pltpu.VMEM((n // 2, tok, width), bf16),
            pltpu.VMEM((n // 8, tok, width), bf16),
            pltpu.VMEM((n // 8, tok, width), bf16),
            pltpu.VMEM((n // 4, tok, width), bf16),
            pltpu.VMEM((n // 4, tok, width), bf16),
            pltpu.VMEM((n // 4, tok, width), bf16),
            pltpu.VMEM((2, tok, width), bf16),
            pltpu.VMEM((2, tok, width), bf16),
            pltpu.VMEM((tok, width), bf16),
            pltpu.SemaphoreType.DMA((feats // chunk,)),
            pltpu.SemaphoreType.DMA((slots,)),
            pltpu.SemaphoreType.DMA,
            pltpu.SemaphoreType.DMA((26,)),
            pltpu.SemaphoreType.DMA((26,)),
        ],
        compiler_params=pltpu.CompilerParams(
            collective_id=0, has_side_effects=True, vmem_limit_bytes=57 * 2**20
        ),
    )(features, fc_weight, centers, labels[None])
    return pl.pallas_call(
        last_kernel,
        out_shape=(
            jax.ShapeDtypeStruct((tok,), f32),
            jax.ShapeDtypeStruct((classes, width), bf16),
            jax.ShapeDtypeStruct((part, width), f32),
        ),
        in_specs=[vmem, vmem, vmem, vmem],
        out_specs=(vmem, hbm, hbm),
        scratch_shapes=[pltpu.VMEM((part, width), f32), pltpu.SemaphoreType.DMA((2,))],
        compiler_params=pltpu.CompilerParams(vmem_limit_bytes=8 * 2**20),
    )(gc, spread, grads, loss)


def solution(mesh):
    placed = (P("cls", None), P(), P("cls", None), P())
    return jax.shard_map(
        on_device,
        mesh=mesh,
        in_specs=placed,
        out_specs=(P("cls"), P("cls", None), P("cls", None)),
        check_vma=False,
    )
```
